256 devices in a mesh: ens: 2 (over z_lo), ctx: 16 (over y, x), group: 8 (over z_hi, core).
Axes of the slice: x: 4, y: 4, z: 8 (z_hi: 4, z_lo: 2; z = z_hi * 2 + z_lo), core: 2. Of those that a mesh axis runs over, the one named last changes fastest.
Arguments:
- latents: bfloat16 [32, 4096, 512], P('ens', ('ctx', 'group')), parts along dimension 0, may hold values from -6 to 6
- rotary_rows: bfloat16 [32, 4096, 64], P('ens', ('ctx', 'group')), parts along dimension 0, may hold values from -6 to 6
- latent_gain: float32 [512], replicated, may hold values from 0.25 to 1.75
- key_up: bfloat16 [1024, 16, 128], P('ens', 'group'), parts along dimension 0, may hold values from -0.25 to 0.25
- value_up: bfloat16 [1024, 16, 128], P('ens', 'group'), parts along dimension 0, may hold values from -0.25 to 0.25
Outputs:
- stored_keys: bfloat16 [32, 16, 192, 4096], P(('ens', 'ctx'), 'group'), parts along dimension 0
- stored_values: bfloat16 [32, 4096, 16, 128], P(('ens', 'ctx'), None, 'group'), parts along dimension 0
The draws below stay inside these ranges and needn't reach their ends.
There are 2 independent parts, one for each index of `ens`. The reference program is written for one: setup_inputs(seed, part) draws one part's arguments, and reference() takes and returns one part's arrays. A program takes and returns all parts, laid end to end along the dimension named above; an argument that names none is the same for every part. Nothing has to cross between parts.
All inputs are finite; a program needn't handle non-finite values.
Results may differ from the reference program's by a relative error of at most 0.0049.
Values may be sent and summed in bfloat16 or wider, within the bound.
No kernel may reach another device: no remote copies, remote signals or barrier semaphores. Data moves between devices by JAX's collectives and lax.ppermute only.
A program may use at most 64 MiB of HBM per device.

```python
import jax
import jax.numpy as jnp
from jax import lax

BATCH = 16
LENGTH = 4096
HEADS = 16
LATENT = 512
KEY_PART = 128
ROTARY = 64
VALUE_SIZE = 128


def levels(key, extent, split, low, top_value):
    loudness, own = 1.0, jax.random.fold_in(key, 6)
    for axis_at, shards_of in split:
        steps = jnp.exp(jax.random.uniform(jax.random.fold_in(own, axis_at), (shards_of,), jnp.float32, low / len(split), top_value / len(split)))
        loudness = loudness * jnp.repeat(steps, extent[axis_at] // shards_of).reshape([-1 if axis == axis_at else 1 for axis in range(len(extent))])
    return loudness


def gaussian(own_key, dims, width, reach, split=(), dtype=jnp.bfloat16):
    array = jax.random.normal(own_key, dims, jnp.float32) * width
    if len(split) > 0:
        array = levels(own_key, dims, split, -0.22, 0.18) * array
    return jnp.clip(array, min=-reach, max=reach).astype(dtype)


def setup_inputs(seed: int = 0, part: int = 0) -> dict:
    arg_keys = jax.random.split(jax.random.key(seed), 6)
    own_keys = jax.random.split(jax.random.fold_in(arg_keys[5], part), 6)
    latents = gaussian(own_keys[0], (BATCH, LENGTH, LATENT), 1.0, 6.0, ((1, 128),))
    rotary_rows = gaussian(own_keys[1], (BATCH, LENGTH, ROTARY), 1.0, 6.0, ((1, 128),))
    latent_gain = jnp.clip(1.0 + 0.15 * jax.random.normal(arg_keys[2], (LATENT,), jnp.float32), 0.25, 1.75)
    key_up = gaussian(own_keys[3], (LATENT, HEADS, KEY_PART), LATENT ** -0.5, 0.25, ((1, 8),))
    value_up = gaussian(own_keys[4], (LATENT, HEADS, VALUE_SIZE), LATENT ** -0.5, 0.25, ((1, 8),))
    return dict(latents=latents, rotary_rows=rotary_rows, latent_gain=latent_gain, key_up=key_up, value_up=value_up)


def root_norm(vectors, row_gain):
    return vectors * lax.rsqrt(lax.optimization_barrier(jnp.mean(vectors * vectors, axis=-1, keepdims=True)) + 1e-06) * row_gain

def reference(latents, rotary_rows, latent_gain, key_up, value_up):
    rows_ready = root_norm(latents.astype(jnp.float32), latent_gain).astype(jnp.bfloat16)
    rows_ready = lax.optimization_barrier(rows_ready)

    def expand_one(one):
        rows_one, rotary_one = one
        wide_keys = jnp.einsum('tr,rhk->thk', rows_one.astype(jnp.float32), key_up.astype(jnp.float32)).astype(jnp.bfloat16)
        shared = jnp.broadcast_to(rotary_one[:, None], (LENGTH, HEADS, ROTARY))
        wide_values = jnp.einsum('tr,rhk->thk', rows_one.astype(jnp.float32), value_up.astype(jnp.float32)).astype(jnp.bfloat16)
        return (jnp.concatenate([wide_keys, shared], axis=-1), wide_values)
    stored_keys, stored_values = lax.map(expand_one, (rows_ready, rotary_rows))
    stored_keys = jnp.transpose(stored_keys, (0, 2, 3, 1))
    return (stored_keys, stored_values)
```

```python
import functools

import jax
import jax.numpy as jnp
from jax import lax
from jax.experimental import pallas as pl
from jax.experimental.pallas import tpu as pltpu
from jax.sharding import PartitionSpec as P


BF16 = jnp.bfloat16
F32 = jnp.float32


def pack_kernel(lat_ref, rot_ref, gain_ref, a_ref, b_ref):
    rows = lat_ref[...].astype(F32)
    scale = lax.rsqrt(jnp.mean(rows * rows, axis=-1, keepdims=True) + 1e-06)
    ready = (rows * scale * gain_ref[...]).astype(BF16)
    for j in range(2):
        a_ref[:, 32 * j : 32 * (j + 1), :] = ready[:, :, 128 * j : 128 * (j + 1)]
    for j in range(2):
        b_ref[:, 32 * j : 32 * (j + 1), :] = ready[:, :, 128 * (j + 2) : 128 * (j + 3)]
    rot = rot_ref[...]
    b_ref[:, 64:80, 0:64] = rot[:, 0:16, :]
    b_ref[:, 64:80, 64:128] = rot[:, 16:32, :]


def pack(latents, rotary, gain):
    return pl.pallas_call(
        pack_kernel,
        out_shape=(
            jax.ShapeDtypeStruct((16, 64, 128), BF16),
            jax.ShapeDtypeStruct((16, 80, 128), BF16),
        ),
        compiler_params=pltpu.CompilerParams(vmem_limit_bytes=16 << 20),
        name="pack",
    )(latents, rotary, gain.reshape(1, 1, 512))


STEP = 4


def expand_kernel(where_ref, *refs):
    pieces, (wk_ref, wv_ref, keys_ref, values_ref, rows, turned, paired) = refs[:16], refs[16:]
    eye = (
        lax.broadcasted_iota(jnp.int32, (64, 64), 0) == lax.broadcasted_iota(jnp.int32, (64, 64), 1)
    ).astype(BF16)
    for c in range(STEP):
        for g in range(8):
            a_ref, b_ref = pieces[2 * g], pieces[2 * g + 1]
            at = pl.multiple_of(where_ref[g], 32)
            for j in range(2):
                rows[pl.ds(at, 32), 128 * j : 128 * (j + 1)] = a_ref[c, 32 * j : 32 * (j + 1), :]
                rows[pl.ds(at, 32), 128 * (j + 2) : 128 * (j + 3)] = b_ref[
                    c, 32 * j : 32 * (j + 1), :
                ]
            rot = b_ref[c, 64:80, :]
            turned[pl.ds(at, 16), :] = rot[:, 0:64]
            turned[pl.ds(at + 16, 16), :] = rot[:, 64:128]
        whole = rows[...]
        lanes = slice(256 * c, 256 * (c + 1))
        wide = lax.dot_general(
            wk_ref[...], whole, (((1,), (1,)), ((), ())), preferred_element_type=F32
        ).astype(BF16)
        shared = lax.dot_general(
            eye, turned[...], (((1,), (1,)), ((), ())), preferred_element_type=F32
        ).astype(BF16)
        for h in range(2):
            keys_ref[h, 0:128, lanes] = wide[128 * h : 128 * (h + 1), :]
            keys_ref[h, 128:192, lanes] = shared
        out = jnp.dot(whole, wv_ref[...], preferred_element_type=F32)
        paired[pl.ds(0, 256, stride=2), :] = out[:, 0:128]
        paired[pl.ds(1, 256, stride=2), :] = out[:, 128:256]
        values_ref[512 * c : 512 * (c + 1), :] = paired[...].astype(BF16)


def expand(where, pieces, wk, wv):
    grid_spec = pltpu.PrefetchScalarGridSpec(
        num_scalar_prefetch=1,
        grid=(16 // STEP,),
        in_specs=[
            pl.BlockSpec((STEP, p.shape[1], 128), lambda i, w: (i, 0, 0)) for p in pieces
        ]
        + [
            pl.BlockSpec((256, 512), lambda i, w: (0, 0)),
            pl.BlockSpec((512, 256), lambda i, w: (0, 0)),
        ],
        out_specs=[
            pl.BlockSpec((2, 192, 256 * STEP), lambda i, w: (0, 0, i)),
            pl.BlockSpec((512 * STEP, 128), lambda i, w: (i, 0)),
        ],
        scratch_shapes=[
            pltpu.VMEM((256, 512), BF16),
            pltpu.VMEM((256, 64), BF16),
            pltpu.VMEM((512, 128), F32),
        ],
    )
    return pl.pallas_call(
        expand_kernel,
        grid_spec=grid_spec,
        out_shape=(
            jax.ShapeDtypeStruct((2, 192, 4096), BF16),
            jax.ShapeDtypeStruct((8192, 128), BF16),
        ),
        compiler_params=pltpu.CompilerParams(vmem_limit_bytes=24 << 20),
        cost_estimate=pl.CostEstimate(
            flops=2 * 4096 * 512 * 512, bytes_accessed=11 << 20, transcendentals=0
        ),
        name="expand",
    )(where, *pieces, wk, wv)


def along(step, other_core=False):
    return [
        (2 * z + c, 2 * ((z + step) % 4) + ((1 - c) if other_core else c))
        for z in range(4)
        for c in range(2)
    ]


def shift(x, step):
    return lax.ppermute(x, "group", along(step))


def swap(x):
    return lax.ppermute(x, "group", along(0, True))


def to_sequences(x):
    return lax.all_to_all(x, "ctx", 0, 0, tiled=True)


def per_device(latents, rotary_rows, latent_gain, key_up, value_up):
    a, b = pack(latents, rotary_rows, latent_gain)
    wk = key_up.transpose(1, 2, 0).reshape(256, 512)
    wv = value_up.reshape(512, 256)
    here, core = lax.axis_index("group") // 2, lax.axis_index("group") % 2

    def around(x):
        left, right = shift(x, 1), shift(x, -1)
        return left, right

    def across(left, right):
        return jnp.concatenate([shift(left[:8], 1), shift(right[8:], -1)], axis=0)

    a = to_sequences(a)
    a_left, a_right = around(a)
    b = to_sequences(b)
    b_left, b_right = around(b)
    a_far = across(a_left, a_right)
    b_far = across(b_left, b_right)
    pieces, where = [], []
    for z, pa, pb in ((0, a, b), (3, a_left, b_left), (1, a_right, b_right), (2, a_far, b_far)):
        for other in range(2):
            pieces += [swap(pa), swap(pb)] if other else [pa, pb]
            where.append((((here + z) % 4) * 2 + (core + other) % 2) * 32)
    keys, values = expand(jnp.stack(where).astype(jnp.int32), pieces, wk, wv)
    return keys.reshape(1, 2, 192, 4096), values.reshape(1, 4096, 2, 128)


def solution(mesh):
    in_specs = (
        P("ens", ("ctx", "group"), None),
        P("ens", ("ctx", "group"), None),
        P(),
        P("ens", "group", None),
        P("ens", "group", None),
    )
    out_specs = (P(("ens", "ctx"), "group", None, None), P(("ens", "ctx"), None, "group", None))
    return jax.shard_map(
        per_device, mesh=mesh, in_specs=in_specs, out_specs=out_specs, check_vma=False
    )
```

```python
import jax
import jax.numpy as jnp
from jax import lax
from jax.experimental import pallas as pl
from jax.experimental.pallas import tpu as pltpu
from jax.sharding import PartitionSpec as P


BF16 = jnp.bfloat16
F32 = jnp.float32


A_LINES, B_LINES = 32, 112


def pack_kernel(lat_hbm, rot_hbm, gain_hbm, a_ref, b_ref, lat_ref, rot_ref, gain_ref, sems):
    copies = [
        pltpu.make_async_copy(src, dst, sems.at[i])
        for i, (src, dst) in enumerate(
            ((lat_hbm, lat_ref), (rot_hbm, rot_ref), (gain_hbm, gain_ref))
        )
    ]
    for copy in copies:
        copy.start()
    for copy in copies:
        copy.wait()
    rows = lat_ref[...].astype(F32)
    scale = lax.rsqrt(jnp.mean(rows * rows, axis=-1, keepdims=True) + 1e-06)
    ready = (rows * scale * gain_ref[...]).astype(BF16)
    a_ref[...] = ready[:, :, 0:128]
    for j in range(3):
        b_ref[:, 32 * j : 32 * (j + 1), :] = ready[:, :, 128 * (j + 1) : 128 * (j + 2)]
    rot = rot_ref[...]
    b_ref[:, 96:112, 0:64] = rot[:, 0:16, :]
    b_ref[:, 96:112, 64:128] = rot[:, 16:32, :]


def pack(latents, rotary, gain):
    return pl.pallas_call(
        pack_kernel,
        in_specs=[pl.BlockSpec(memory_space=pltpu.HBM)] * 3,
        out_shape=(
            pltpu.VMEM((16, A_LINES, 128), BF16),
            pltpu.VMEM((16, B_LINES, 128), BF16),
        ),
        scratch_shapes=[
            pltpu.VMEM((16, 32, 512), BF16),
            pltpu.VMEM((16, 32, 64), BF16),
            pltpu.VMEM((1, 1, 512), F32),
            pltpu.SemaphoreType.DMA((3,)),
        ],
        compiler_params=pltpu.CompilerParams(vmem_limit_bytes=66453504),
        name="pack",
    )(latents, rotary, gain.reshape(1, 1, 512))


def join_kernel(*refs):
    *parts, out_ref = refs
    at = 0
    for part in parts:
        lines = part.shape[1]
        out_ref[:, at : at + lines, :] = part[...]
        at += lines


def join(parts):
    lines = sum(p.shape[1] for p in parts)
    return pl.pallas_call(
        join_kernel,
        out_shape=pltpu.VMEM((16, lines, 128), BF16),
        compiler_params=pltpu.CompilerParams(vmem_limit_bytes=8 << 20),
        name="join",
    )(*parts)


def cut_kernel(slots, b_ref, out_ref):
    out_ref[...] = b_ref[slots, :, :]


def cut(b, slots):
    return pl.pallas_call(
        lambda *refs: cut_kernel(slots, *refs),
        in_specs=[pl.BlockSpec(memory_space=pltpu.VMEM)],
        out_shape=pltpu.VMEM((8, B_LINES, 128), BF16),
        compiler_params=pltpu.CompilerParams(vmem_limit_bytes=8 << 20),
        name="cut",
    )(b)


STEPS, SLOTS = 8, 4


def expand_kernel(last, parts, *refs):
    a_refs, b_own, b_first, b_second = refs[0:2], refs[2:4], refs[4:6], refs[6:8]
    b_far, refs = (refs[8:10], refs[10:]) if last else (None, refs[8:])
    wk_ref, wv_ref = refs[0:2]
    keys_hbm, values_hbm, turned, paired, kbuf, vbuf, sems = refs[-7:]
    group = lax.axis_index("group")
    core, odd = lax.bitwise_and(group, 1), lax.bitwise_and(lax.shift_right_logical(group, 1), 1)
    half = lax.bitwise_xor(lax.shift_right_logical(group, 2), last)
    eye = (
        lax.broadcasted_iota(jnp.int32, (64, 64), 0) == lax.broadcasted_iota(jnp.int32, (64, 64), 1)
    ).astype(BF16)

    def leave(step, slot):
        out = []
        for c in range(2):
            block = 2 * (2 * step + c) + half
            lanes = pl.ds(pl.multiple_of(block * 128, 128), 128)
            rows = pl.ds(pl.multiple_of(block * 256, 256), 256)
            out.append(
                pltpu.make_async_copy(
                    kbuf.at[slot, c], keys_hbm.at[:, :, lanes], sems.at[slot, c]
                )
            )
            out.append(
                pltpu.make_async_copy(
                    vbuf.at[slot, c], values_hbm.at[rows], sems.at[slot, 2 + c]
                )
            )
        return out

    def run(is_odd, on_core):
        from_left = is_odd != last
        pieces = []
        for group in range(4):
            i = (group % 2) ^ on_core
            if group // 2 == is_odd:
                pieces.append((i, A_LINES * (2 if last else 0), None))
            elif from_left == (i == on_core):
                pieces.append((i, A_LINES, b_first[i]))
            else:
                pieces.append((i, A_LINES * 3, b_second[i]))

        def one(step, carry, part):
            slot = lax.rem(step, SLOTS)

            @pl.when(step >= parts[0] * (STEPS // 2) + SLOTS)
            def _():
                for copy in leave(step - SLOTS, slot):
                    copy.wait()

            def from_b(i, ref, c):
                if ref is not None:
                    return ref, 2 * step + c
                if last:
                    return b_far[i], 2 * step + c - 8 * part
                return b_own[i], 2 * step + c

            def lines(i, top, beside, c):
                ref, at = from_b(i, beside, c)
                return jnp.concatenate(
                    [a_refs[i][2 * step + c, top : top + 32, :]]
                    + [ref[at, 32 * j : 32 * (j + 1), :] for j in range(3)],
                    axis=1,
                )

            def whole():
                return jnp.concatenate(
                    [lines(*piece, c) for c in range(2) for piece in pieces], axis=0
                )

            for c in range(2):
                for g, (i, _, beside) in enumerate(pieces):
                    ref, at = from_b(i, beside, c)
                    rot = ref[at, 96:112, :]
                    at = 128 * c + 32 * g
                    turned[at : at + 16, :] = rot[:, 0:64]
                    turned[at + 16 : at + 32, :] = rot[:, 64:128]
            wide = lax.dot_general(
                wk_ref[...], whole(), (((1,), (1,)), ((), ())), preferred_element_type=F32
            ).astype(BF16)
            shared = lax.dot_general(
                eye, turned[...], (((1,), (1,)), ((), ())), preferred_element_type=F32
            ).astype(BF16)
            for c in range(2):
                lanes = slice(128 * c, 128 * (c + 1))
                for h in range(2):
                    kbuf[slot, c, h, 0:128, :] = wide[128 * h : 128 * (h + 1), lanes]
                    kbuf[slot, c, h, 128:192, :] = shared[:, lanes]
            wv = jnp.concatenate([wv_ref[0], wv_ref[1]], axis=1)
            out = jnp.dot(whole(), wv, preferred_element_type=F32)
            paired[pl.ds(0, 256, stride=2), :] = out[:, 0:128]
            paired[pl.ds(1, 256, stride=2), :] = out[:, 128:256]
            for c in range(2):
                vbuf[slot, c] = paired[256 * c : 256 * (c + 1), :].astype(BF16)
            for copy in leave(step, slot):
                copy.start()
            return carry

        for part in parts:
            first = part * (STEPS // 2)
            lax.fori_loop(first, first + STEPS // 2, lambda s, x: one(s, x, part), 0)

    for is_odd in range(2):
        for on_core in range(2):
            pl.when(jnp.logical_and(odd == is_odd, core == on_core))(
                lambda is_odd=is_odd, on_core=on_core: run(is_odd, on_core)
            )
    end = (parts[-1] + 1) * (STEPS // 2)
    for step in range(end - SLOTS, end):
        for copy in leave(step, step % SLOTS):
            copy.wait()


def expand(last, parts, a_pieces, own, first, second, far, wk, wv, before):
    pieces = (*a_pieces, *own, *first, *second, *far, wk, wv)
    hbm = pl.BlockSpec(memory_space=pl.ANY)
    vmem = pl.BlockSpec(memory_space=pltpu.VMEM)
    count = len(pieces)
    return pl.pallas_call(
        lambda *refs: expand_kernel(last, parts, *refs),
        in_specs=[vmem] * len(pieces) + [hbm] * len(before),
        out_specs=[hbm, hbm],
        out_shape=(
            jax.ShapeDtypeStruct((2, 192, 4096), BF16),
            jax.ShapeDtypeStruct((8192, 128), BF16),
        ),
        scratch_shapes=[
            pltpu.VMEM((256, 64), BF16),
            pltpu.VMEM((512, 128), F32),
            pltpu.VMEM((SLOTS, 2, 2, 192, 128), BF16),
            pltpu.VMEM((SLOTS, 2, 256, 128), BF16),
            pltpu.SemaphoreType.DMA((SLOTS, 4)),
        ],
        input_output_aliases={count: 0, count + 1: 1} if before else {},
        compiler_params=pltpu.CompilerParams(vmem_limit_bytes=9 << 20),
        cost_estimate=pl.CostEstimate(
            flops=2048 * 512 * 512 * len(parts), bytes_accessed=5 << 20, transcendentals=0
        ),
        name="expand",
    )(*pieces, *before)


def along(step, other_core=False):
    return [
        (2 * z + c, 2 * ((z + step) % 4) + ((1 - c) if other_core else c))
        for z in range(4)
        for c in range(2)
    ]


def ring(x, step):
    pairs = [(2 * z + c, 2 * ((z + (1 - 2 * c) * step) % 4) + c) for z in range(4) for c in range(2)]
    return lax.ppermute(x, "group", pairs)


def swap(x):
    return lax.ppermute(x, "group", along(0, True))


def to_sequences(x):
    return lax.all_to_all(x, "ctx", 0, 0, tiled=True)


def staged(latents, rotary_rows, latent_gain, key_up, value_up):
    a, b = pack(latents, rotary_rows, latent_gain)
    wk = key_up.transpose(1, 2, 0).reshape(256, 512)
    wv = value_up.transpose(1, 0, 2)

    a_first, a_second, a_far = ring(a, 1), ring(a, -1), ring(a, 2)
    b = to_sequences(b)
    b_first, b_second = ring(b, 1), ring(b, -1)
    a_all = join((a, a_first, a_far, a_second))
    a_all = to_sequences(a_all)
    low, high = cut(b_first, slice(0, 8)), cut(b_second, slice(8, 16))
    far_low, far_high = ring(low, 1), ring(high, -1)
    a_pieces = (a_all, swap(a_all))
    b_with, wk, wv = lax.optimization_barrier((b, wk, wv))
    near = ((b, swap(b_with)), (b_first, swap(b_first)), (b_second, swap(b_second)))
    outs = ()
    outs = expand(0, (0, 1), a_pieces, *near, (), wk, wv, outs)
    far = (far_low, swap(far_low))
    outs = expand(1, (0,), a_pieces, *near, far, wk, wv, outs)
    far = (far_high, swap(far_high))
    outs = expand(1, (1,), a_pieces, *near, far, wk, wv, outs)
    keys, values = outs
    return keys.reshape(1, 2, 192, 4096), values.reshape(1, 4096, 2, 128)


def solution(mesh):
    in_specs = (
        P("ens", ("ctx", "group"), None),
        P("ens", ("ctx", "group"), None),
        P(),
        P("ens", "group", None),
        P("ens", "group", None),
    )
    out_specs = (P(("ens", "ctx"), "group", None, None), P(("ens", "ctx"), None, "group", None))
    return jax.shard_map(staged, mesh=mesh, in_specs=in_specs, out_specs=out_specs, check_vma=False)
```
